32 devices in a mesh: ctx: 8 (over z, x), rep: 4 (over y, core).
Axes of the slice: x: 2, y: 2, z: 4, core: 2. Of those that a mesh axis runs over, the one named last changes fastest.
Arguments:
- latents: bfloat16 [131072, 576], P(('ctx', 'rep')), may hold values from -6 to 6
- queries: bfloat16 [64, 73728], P('rep', 'ctx'), may hold values from -4000 to 4000, as said below
- hot_ids: int32 [16], P('ctx'), may hold values from 0 to 15, as said below
- lengths: int32 [64], P('rep'), may hold values from 65536 to 131072
Outputs:
- attended: bfloat16 [64, 65536], P('rep', 'ctx')
The draws below stay inside these ranges and needn't reach their ends.
Inputs may be any that keep to these rules, and one draw needn't show every extreme that they name: `queries`: query entries lie in the stated range. `hot_ids`: entries g * 2 to (g + 1) * 2 - 1 are distinct block numbers within group g.
All inputs are finite; a program needn't handle non-finite values.
Results may differ from the reference program's by a relative error of at most 0.0031.
Values may be sent and summed in bfloat16 or wider, within the bound.
A program may use at most 128 MiB of HBM per device.

```python
import jax
import jax.numpy as jnp
from jax import lax

H = 128
LAT = 512
ROPE = 64
QK = 192
BLK = 1024
HOT_GRP = 2
BPG = 16
CTX = 131072
NQ = 64
N_CTX = 8


def hot_table(key):
    sub_keys = jax.random.split(jax.random.fold_in(key, 101), N_CTX)
    picked_ids = jax.vmap(lambda one_key: jax.random.permutation(one_key, BPG)[:HOT_GRP])(sub_keys)
    return picked_ids.reshape(-1).astype(jnp.int32)


def block_rows(key, block_number):
    row_width = LAT + ROPE
    block_key = jax.random.fold_in(jax.random.fold_in(key, 202), block_number)
    return jnp.clip(jax.random.normal(block_key, (BLK, row_width), jnp.float32), -6.0, 6.0)


def probe_target(pair_index):
    return 120.0 + 45.0 * pair_index


def apply_pairs(pair_rows):
    for pair_index in range(4):
        upper_row = 2 * pair_index
        pair_rows = pair_rows.at[upper_row, LAT].set(1.0)
        energy = jnp.sum(pair_rows[upper_row, LAT:] * pair_rows[upper_row, LAT:])
        lower_entry = 1.0 - 2.0 * energy / probe_target(pair_index)
        pair_rows = pair_rows.at[upper_row + 1, LAT:].set(pair_rows[upper_row, LAT:])
        pair_rows = pair_rows.at[upper_row + 1, LAT].set(lower_entry)
    return pair_rows


def draw_hot_ids(key, part):
    return hot_table(key)


def draw_latents(key, part):
    row_width = LAT + ROPE
    all_blocks = jax.vmap(lambda number: block_rows(key, number))(jnp.arange(CTX // BLK, dtype=jnp.int32))
    first_block = hot_table(key)[0]
    all_blocks = all_blocks.at[first_block].set(apply_pairs(all_blocks[first_block]))
    return all_blocks.reshape(CTX, row_width).astype(jnp.bfloat16)


def draw_queries(key, part):
    row_width = LAT + ROPE
    query_draw = 1.5 * jnp.clip(jax.random.normal(jax.random.fold_in(key, 303), (NQ, H, row_width), jnp.float32), -6.0, 6.0)
    pair_rows = apply_pairs(block_rows(key, hot_table(key)[0]))
    for pair_index in range(4):
        rotary_part = pair_rows[2 * pair_index, LAT:]
        energy = jnp.sum(rotary_part * rotary_part)
        strength = probe_target(pair_index) * QK ** 0.5 / energy
        probe_row = jnp.zeros((row_width,), jnp.float32).at[LAT:].set(strength * rotary_part)
        query_draw = query_draw.at[pair_index * (NQ // 4), pair_index].set(probe_row)
    return query_draw.reshape(NQ, H * row_width).astype(jnp.bfloat16)


def set_ends(values, own_key, low, high):
    longest = values.shape.index(max(values.shape))
    spots = []
    for shift in (0, 1):
        where = [jax.random.randint(jax.random.fold_in(own_key, axis), (), 0, length) for axis, length in enumerate(values.shape)]
        where[longest] = (where[longest] + shift) % values.shape[longest]
        spots.append(tuple(where))
    return values.at[spots[0]].set(low).at[spots[1]].set(high)


def setup_inputs(seed: int = 0) -> dict:
    streams_of = jax.random.split(jax.random.key(seed), 5)
    latents = draw_latents(jax.random.fold_in(streams_of[4], 71), 0)
    queries = draw_queries(jax.random.fold_in(streams_of[4], 71), 0)
    hot_ids = draw_hot_ids(jax.random.fold_in(streams_of[4], 71), 0)
    lengths = set_ends(jax.random.randint(streams_of[3], (NQ,), CTX // 2, CTX + 1), jax.random.fold_in(streams_of[3], 1), CTX // 2, CTX).astype(jnp.int32)
    return {"latents": latents, "queries": queries, "hot_ids": hot_ids, "lengths": lengths}


def group_partials(query_heads, key_rows, row_index, lengths, score_scale):
    scores = jnp.einsum("qhw,kw->qhk", query_heads.astype(jnp.float32), key_rows.astype(jnp.float32)) * score_scale
    visible = row_index[None, None, :] < lengths[:, None, None]
    peak_score = jnp.max(jnp.where(visible, scores, -1e30), axis=2)
    exponent = jnp.where(visible, scores - peak_score[:, :, None], -1e30)
    weights = jnp.exp(exponent).astype(jnp.bfloat16)
    totals = jnp.sum(weights.astype(jnp.float32), axis=2)
    numerators = jnp.einsum("qhk,kl->qhl", weights.astype(jnp.float32), key_rows[:, :LAT].astype(jnp.float32))
    return numerators, peak_score, totals


def reference(latents, queries, hot_ids, lengths):
    row_width = LAT + ROPE
    score_scale = QK ** -0.5
    query_heads = queries.reshape(NQ, H, row_width)
    blocks = latents.reshape(N_CTX, BPG, BLK, row_width)
    hot_matrix = hot_ids.reshape(N_CTX, HOT_GRP)
    offsets = jnp.arange(BLK, dtype=jnp.int32)

    def fold(running, group_index):
        overall, numer_run, total_run = running
        chosen = hot_matrix[group_index]
        key_rows = blocks[group_index][chosen].reshape(HOT_GRP * BLK, row_width)
        row_index = ((group_index * BPG + chosen)[:, None] * BLK + offsets[None, :]).reshape(-1).astype(jnp.int32)
        numerators, peak_score, totals = group_partials(query_heads, key_rows, row_index, lengths, score_scale)
        new_overall = jnp.maximum(overall, peak_score)
        old_factor = jnp.exp(overall - new_overall)
        new_factor = jnp.exp(peak_score - new_overall)
        numer_run = numer_run * old_factor[..., None] + numerators * new_factor[..., None]
        total_run = total_run * old_factor + totals * new_factor
        return (new_overall, numer_run, total_run), None

    initial = (jnp.full((NQ, H), -1e30, jnp.float32), jnp.zeros((NQ, H, LAT), jnp.float32), jnp.zeros((NQ, H), jnp.float32))
    (overall, numer_run, total_run), _ = lax.scan(fold, initial, jnp.arange(N_CTX, dtype=jnp.int32))
    return (numer_run / total_run[..., None]).reshape(NQ, H * LAT).astype(jnp.bfloat16)
```

```python
import functools

import jax
import jax.numpy as jnp
from jax import lax
from jax.experimental import pallas as pl
from jax.experimental.pallas import tpu as pltpu
from jax.sharding import PartitionSpec as P

H = 128
LAT = 512
ROPE = 64
QK = 192
BLK = 1024
HOT_GRP = 2
LANES = 128
PIECES = 8
SPAN = 512
MESH = pl.DeviceIdType.MESH


def kernel(
    n_ctx, n_rep, cand_ref, own_q_ref, base_ref, limit_ref, out_ref,
    from_core, merged, from_far, keys, heads, base_near, stat_send, stat_recv,
    part_send, part_recv, part_own, acc, peak_ref, total_ref, send_sem, recv_sem,
):
    outer = n_ctx // 2
    rows = own_q_ref.shape[0]
    piece = BLK // PIECES
    group = lax.axis_index("ctx")
    rep = lax.axis_index("rep")
    side = lax.rem(rep, 2)
    core = {"rep": rep + 1 - 2 * side}
    far = {"rep": lax.rem(rep + n_rep // 2, n_rep)}
    near = {"ctx": group + 1 - 2 * lax.rem(group, 2)}

    def line(d):
        return {"ctx": lax.rem(group + 2 * d, n_ctx)}

    barrier = pltpu.get_barrier_semaphore()
    for target in (core, far, near):
        pl.semaphore_signal(barrier, inc=1, device_id=target, device_id_type=MESH)

    @pl.loop(1, outer)
    def _(d):
        pl.semaphore_signal(barrier, inc=1, device_id=line(d), device_id_type=MESH)

    pl.semaphore_wait(barrier, outer + 2)

    def copy(src, dst, sem, target):
        return pltpu.make_async_remote_copy(
            src_ref=src, dst_ref=dst, send_sem=send_sem.at[sem], recv_sem=recv_sem.at[sem],
            device_id=target, device_id_type=MESH,
        )

    def cut(k):
        return pl.ds(k * piece, piece)

    def to_core(k):
        return copy(cand_ref.at[1 - side, cut(k)], from_core.at[cut(k)], k, core)

    def to_far(k):
        return copy(merged.at[cut(k)], from_far.at[cut(k)], PIECES + k, far)

    def to_near(k):
        return copy(keys.at[0, side, cut(k)], keys.at[1, side, cut(k)], 2 * PIECES + k, near)

    def share(where, slot, k):
        ref = keys.at[where, slot, cut(k)]
        return copy(ref, ref, (3 + where) * PIECES + k, core)

    first = 5 * PIECES
    base_copy = copy(base_ref, base_near, first, near)

    def query_copy(d):
        return copy(own_q_ref, heads.at[d], first + d, line(d))

    def part_copy(d):
        return copy(part_send.at[d], part_recv.at[d], first + outer + d, line(outer - d))

    def stat_copy(d):
        return copy(stat_send.at[d], stat_recv.at[d], first + 2 * outer + d, line(outer - d))

    for k in range(PIECES):
        to_core(k).start()
    base_copy.start()

    @pl.loop(1, outer)
    def _(d):
        query_copy(d).start()

    for k in range(PIECES):
        to_core(k).wait_recv()
        merged[cut(k), :] = cand_ref[side, cut(k), :] + from_core[cut(k), :]
        to_far(k).start()

    limits = limit_ref[...]

    def begin():
        acc[...] = jnp.zeros_like(acc)
        peak_ref[...] = jnp.full_like(peak_ref, -1e30)
        total_ref[...] = jnp.zeros_like(total_ref)

    def absorb(query_rows, where, slot, start, base):
        key_rows = keys[where, slot, pl.ds(start, SPAN), :]
        score = lax.dot_general(
            query_rows, key_rows, (((1,), (1,)), ((), ())), preferred_element_type=jnp.float32
        ) * (QK ** (-0.5))
        position = base + start + lax.broadcasted_iota(jnp.int32, (1, SPAN), 1)
        visible = position < limits[:, :1]
        old = peak_ref[...]
        new = jnp.maximum(old, jnp.max(jnp.where(visible, score, -1e30), axis=1, keepdims=True))
        weight = jnp.exp(jnp.where(visible, score - new[:, :1], -1e30)).astype(jnp.bfloat16)
        shrink = jnp.exp(old - new)
        peak_ref[...] = new
        total_ref[...] = total_ref[...] * shrink + jnp.sum(
            weight.astype(jnp.float32), axis=1, keepdims=True
        )
        acc[...] = acc[...] * shrink[:, :1] + jnp.dot(
            weight, key_rows[:, :LAT], preferred_element_type=jnp.float32
        )

    def base_of(where, slot):
        ref = base_ref if where == 0 else base_near
        row = ref[slot : slot + 1, :]
        return jnp.concatenate([row] * (SPAN // LANES), axis=1)

    def finish():
        total = total_ref[...]
        lane = lax.broadcasted_iota(jnp.int32, (rows, LANES), 1)
        stats = jnp.where(lane < 4, peak_ref[...], total)
        if rows % LANES:
            stats = jnp.concatenate(
                [stats, jnp.zeros((LANES - rows % LANES, LANES), jnp.float32)], axis=0
            )
        inverse = 1.0 / jnp.maximum(total, 1e-30)
        return acc[...] * inverse[:, :1], jnp.transpose(stats)[:8, :]

    begin()
    own_rows = own_q_ref[...]
    base_copy.wait_recv()

    def pass_on(k):
        to_near(k).wait_recv()
        share(1, side, k).start()

    per_span = SPAN // piece
    for k in range(PIECES):
        to_far(k).wait_recv()
        keys[0, side, cut(k), :] = merged[cut(k), :] + from_far[cut(k), :]
        to_near(k).start()
        share(0, side, k).start()
        if k >= 2:
            pass_on(k - 2)
        share(0, 1 - side, k).wait_recv()
        if k % per_span == per_span - 1:
            start = (k // per_span) * SPAN
            for slot in range(HOT_GRP):
                absorb(own_rows, 0, slot, start, base_of(0, slot))
    for k in range(max(PIECES - 2, 0), PIECES):
        pass_on(k)
    for k in range(PIECES):
        share(1, 1 - side, k).wait_recv()
        if k % per_span == per_span - 1:
            start = (k // per_span) * SPAN
            for slot in range(HOT_GRP):
                absorb(own_rows, 1, slot, start, base_of(1, slot))
    part, stats = finish()
    part_own[...] = part
    stat_recv[0] = stats

    @pl.loop(1, outer)
    def _(d):
        query_copy(d).wait_recv()
        begin()
        query_rows = heads[d]
        for where in range(2):
            for slot in range(HOT_GRP):
                base = base_of(where, slot)
                for start in range(0, BLK, SPAN):
                    absorb(query_rows, where, slot, start, base)
        part, stats = finish()
        stat_send[d] = stats
        part_send[d] = part.astype(jnp.bfloat16)
        stat_copy(d).start()
        part_copy(d).start()

    for k in range(PIECES):
        to_core(k).wait_send()
        to_far(k).wait_send()
        to_near(k).wait_send()
        share(0, side, k).wait_send()
        share(1, side, k).wait_send()
    base_copy.wait_send()

    @pl.loop(1, outer)
    def _(d):
        query_copy(d).wait_send()
        stat_copy(d).wait()

    every = [stat_recv[d] for d in range(outer)]
    overall = functools.reduce(jnp.maximum, [s[:1, :] for s in every])
    shares = [jnp.exp(s[:1, :] - overall) * s[4:5, :] for s in every]
    inverse = 1.0 / functools.reduce(jnp.add, shares)

    def column(d):
        across = jnp.broadcast_to(shares[d] * inverse, (LANES, shares[d].shape[1]))
        return jnp.transpose(across)[:rows, :1]

    acc[...] = part_own[...] * column(0)
    for d in range(1, outer):
        part_copy(d).wait()
        acc[...] += part_recv[d].astype(jnp.float32) * column(d)
    out_ref[...] = acc[...].astype(out_ref.dtype)


def on_device(latents, queries, hot_ids, lengths):
    width = LAT + ROPE
    padded = -(-width // LANES) * LANES
    n_rep = lax.axis_size("rep")
    n_ctx = lax.axis_size("ctx")
    group = lax.axis_index("ctx")
    me = lax.axis_index("rep")
    per_device = latents.shape[0] // BLK
    found = []
    for slot in range(HOT_GRP):
        block = lax.dynamic_slice_in_dim(latents, hot_ids[slot] % per_device * BLK, BLK, 0)
        found.append(jnp.where(hot_ids[slot] // per_device == me, block, jnp.zeros_like(block)))
    cand = jnp.pad(jnp.stack(found), ((0, 0), (0, 0), (0, padded - width)))
    count = queries.shape[0]
    local = queries.shape[1] // width
    rows = count * local
    own_q = jnp.pad(queries.reshape(rows, width), ((0, 0), (0, padded - width)))
    base = (group * (n_rep * per_device) + hot_ids) * BLK
    base = jnp.broadcast_to(jnp.pad(base, (0, 8 - HOT_GRP))[:, None], (8, LANES))
    limit = jnp.broadcast_to(lengths[:, None, None], (count, local, LANES)).reshape(rows, LANES)
    outer = n_ctx // 2
    wide = -(-rows // LANES) * LANES
    sems = 5 * PIECES + 3 * outer
    vmem = pl.BlockSpec(memory_space=pltpu.VMEM)
    bf16, f32 = jnp.bfloat16, jnp.float32
    out = pl.pallas_call(
        functools.partial(kernel, n_ctx, n_rep),
        out_shape=jax.ShapeDtypeStruct((rows, LAT), bf16),
        in_specs=[vmem] * 4,
        out_specs=vmem,
        scratch_shapes=[
            pltpu.VMEM((BLK, padded), bf16),
            pltpu.VMEM((BLK, padded), bf16),
            pltpu.VMEM((BLK, padded), bf16),
            pltpu.VMEM((2, HOT_GRP, BLK, padded), bf16),
            pltpu.VMEM((outer, rows, padded), bf16),
            pltpu.VMEM((8, LANES), jnp.int32),
            pltpu.VMEM((outer, 8, wide), f32),
            pltpu.VMEM((outer, 8, wide), f32),
            pltpu.VMEM((outer, rows, LAT), bf16),
            pltpu.VMEM((outer, rows, LAT), bf16),
            pltpu.VMEM((rows, LAT), f32),
            pltpu.VMEM((rows, LAT), f32),
            pltpu.VMEM((rows, LANES), f32),
            pltpu.VMEM((rows, LANES), f32),
            pltpu.SemaphoreType.DMA((sems,)),
            pltpu.SemaphoreType.DMA((sems,)),
        ],
        compiler_params=pltpu.CompilerParams(
            collective_id=0, has_side_effects=True, vmem_limit_bytes=48 * 1024 * 1024
        ),
    )(cand, own_q, base, limit)
    return out.reshape(count, local * LAT)


def solution(mesh):
    placed = (P(("ctx", "rep"), None), P("rep", "ctx"), P("ctx"), P("rep"))
    return jax.shard_map(
        on_device, mesh=mesh, in_specs=placed, out_specs=P("rep", "ctx"), check_vma=False
    )
```

```python
import functools

import jax
import jax.numpy as jnp
from jax import lax
from jax.experimental import pallas as pl
from jax.experimental.pallas import tpu as pltpu
from jax.sharding import PartitionSpec as P

H = 128
LAT = 512
ROPE = 64
QK = 192
BLK = 1024
HOT_GRP = 2
LANES = 128
PIECES = 8
SPAN = 512
MESH = pl.DeviceIdType.MESH


def kernel(
    n_ctx, n_rep, latent_ref, query_ref, hot_ref, length_ref, out_ref,
    cand, from_core, merged, from_far, keys, heads, base_own, base_near, stat_send, stat_recv,
    part_send, part_recv, acc, peaks, totals, send_sem, recv_sem,
):
    outer = n_ctx // 2
    count = query_ref.shape[0]
    width = latent_ref.shape[0]
    local = query_ref.shape[1] // width
    rows = count * local
    per_device = latent_ref.shape[1] // BLK
    piece = BLK // PIECES
    group = lax.axis_index("ctx")
    rep = lax.axis_index("rep")
    side = lax.rem(rep, 2)
    core = {"rep": rep + 1 - 2 * side}
    far = {"rep": lax.rem(rep + n_rep // 2, n_rep)}
    near = {"ctx": group + 1 - 2 * lax.rem(group, 2)}

    def line(d):
        return {"ctx": lax.rem(group + 2 * d, n_ctx)}

    barrier = pltpu.get_barrier_semaphore()
    for target in (core, far, near):
        pl.semaphore_signal(barrier, inc=1, device_id=target, device_id_type=MESH)

    @pl.loop(1, outer)
    def _(d):
        pl.semaphore_signal(barrier, inc=1, device_id=line(d), device_id_type=MESH)

    def factors(slot):
        hot = jnp.full((1, LANES), hot_ref[slot], jnp.int32)
        return [
            jnp.where(hot == rep * per_device + b, 1.0, 0.0).astype(jnp.bfloat16)
            for b in range(per_device)
        ]

    other_factors = factors(1 - side)
    own_factors = factors(side)

    def held(chosen, k):
        return functools.reduce(
            jnp.add,
            [
                latent_ref[:, b * BLK + k * piece : b * BLK + (k + 1) * piece] * chosen[b]
                for b in range(per_device)
            ],
        )

    cand[0] = held(other_factors, 0)
    pl.semaphore_wait(barrier, outer + 2)

    def copy(src, dst, sem, target):
        return pltpu.make_async_remote_copy(
            src_ref=src, dst_ref=dst, send_sem=send_sem.at[sem], recv_sem=recv_sem.at[sem],
            device_id=target, device_id_type=MESH,
        )

    def to_core(k):
        return copy(cand.at[k], from_core.at[k], k, core)

    def to_far(k):
        return copy(merged.at[k], from_far.at[k], PIECES + k, far)

    def to_near(k):
        return copy(keys.at[0, side, k], keys.at[1, side, k], 2 * PIECES + k, near)

    def share(where, slot, k):
        ref = keys.at[where, slot, k]
        return copy(ref, ref, (3 + where) * PIECES + k, core)

    first = 5 * PIECES
    base_copy = copy(base_own, base_near, first, near)

    def query_copy(d):
        return copy(heads.at[0], heads.at[d], first + d, line(d))

    def part_copy(d):
        return copy(part_send.at[d], part_recv.at[d], first + outer + d, line(outer - d))

    def stat_copy(d):
        return copy(stat_send.at[d], stat_recv.at[d], first + 2 * outer + d, line(outer - d))

    to_core(0).start()
    for k in range(1, PIECES):
        cand[k] = held(other_factors, k)
        to_core(k).start()
    for h in range(local):
        heads[0, h * count : (h + 1) * count, :] = query_ref[:, h * width : (h + 1) * width]
    slot_row = lax.broadcasted_iota(jnp.int32, (8, LANES), 0)
    base = jnp.zeros((8, LANES), jnp.int32)
    for slot in range(HOT_GRP):
        at = (group * (n_rep * per_device) + hot_ref[slot]) * BLK
        base = jnp.where(slot_row == slot, at, base)
    base_own[...] = base

    for k in range(PIECES):
        to_core(k).wait_recv()
        merged[k] = held(own_factors, k) + from_core[k]
        to_far(k).start()
        if k == 0:
            @pl.loop(1, outer)
            def _(d):
                query_copy(d).start()
            base_copy.start()

    query_row = lax.broadcasted_iota(jnp.int32, (count, LANES), 0)
    limit = jnp.zeros((count, LANES), jnp.int32)
    for q in range(count):
        limit = jnp.where(query_row == q, length_ref[q], limit)
    limits = jnp.concatenate([limit] * local, axis=0)[:, :1]

    acc[...] = jnp.zeros_like(acc)
    peaks[...] = jnp.full_like(peaks, -1e30)
    totals[...] = jnp.zeros_like(totals)
    per_span = SPAN // piece

    def absorb(d, where, slot, span):
        key_cols = jnp.concatenate(
            [keys[where, slot, span * per_span + i] for i in range(per_span)], axis=1
        )
        score = jnp.dot(
            heads[d], key_cols, preferred_element_type=jnp.float32
        ) * (QK ** (-0.5))
        ref = base_own if where == 0 else base_near
        base = jnp.concatenate([ref[slot : slot + 1, :]] * (SPAN // LANES), axis=1)
        position = base + span * SPAN + lax.broadcasted_iota(jnp.int32, (1, SPAN), 1)
        visible = position < limits
        score = jnp.where(visible, score, -1e30)
        old = peaks[d]
        new = jnp.maximum(old, jnp.max(score, axis=1, keepdims=True))
        weight = jnp.exp(jnp.where(visible, score - new[:, :1], -1e30)).astype(jnp.bfloat16)
        shrink = jnp.exp(old - new)
        peaks[d] = new
        totals[d] = totals[d] * shrink + jnp.sum(
            weight.astype(jnp.float32), axis=1, keepdims=True
        )
        acc[d] = acc[d] * shrink[:, :1] + lax.dot_general(
            weight, key_cols[:LAT, :], (((1,), (1,)), ((), ())),
            preferred_element_type=jnp.float32,
        )

    def absorb_rest(where, slot, span):
        @pl.loop(1, outer)
        def _(d):
            absorb(d, where, slot, span)

    def finish(d):
        total = totals[d]
        lane = lax.broadcasted_iota(jnp.int32, (rows, LANES), 1)
        stats = jnp.where(lane < 4, peaks[d], total)
        if rows % LANES:
            stats = jnp.concatenate(
                [stats, jnp.zeros((LANES - rows % LANES, LANES), jnp.float32)], axis=0
            )
        inverse = 1.0 / jnp.maximum(total, 1e-30)
        return acc[d] * inverse[:, :1], jnp.transpose(stats)[:8, :]

    def pass_on(k):
        to_near(k).wait_recv()
        share(1, side, k).start()
        share(1, 1 - side, k).wait_recv()

    spans = BLK // SPAN
    waiting = []
    base_copy.wait_recv()
    for k in range(PIECES + 2):
        if k < PIECES:
            to_far(k).wait_recv()
            keys[0, side, k] = merged[k] + from_far[k]
            to_near(k).start()
            share(0, side, k).start()
            share(0, 1 - side, k).wait_recv()
            if k % per_span == per_span - 1:
                for slot in range(HOT_GRP):
                    absorb(0, 0, slot, k // per_span)
                    waiting.append((0, slot, k // per_span))
        if k >= 2:
            pass_on(k - 2)
            if (k - 2) % per_span == per_span - 1 and (k - 2) // per_span < spans - 1:
                for slot in range(HOT_GRP):
                    absorb(0, 1, slot, (k - 2) // per_span)
                    waiting.append((1, slot, (k - 2) // per_span))
        if k == PIECES - 2:
            @pl.loop(1, outer)
            def _(d):
                query_copy(d).wait_recv()
        if k >= PIECES - 2:
            for task in waiting[:2]:
                absorb_rest(*task)
            waiting = waiting[2:]
    for task in waiting:
        absorb_rest(*task)

    @pl.loop(1, outer)
    def _(d):
        for slot in range(HOT_GRP):
            absorb(d, 1, slot, spans - 1)
        part, stats = finish(d)
        stat_send[d] = stats
        part_send[d] = part.astype(jnp.bfloat16)
        stat_copy(d).start()
        part_copy(d).start()

    for slot in range(HOT_GRP):
        absorb(0, 1, slot, spans - 1)
    part, stats = finish(0)
    acc[0] = part
    stat_recv[0] = stats

    for k in range(PIECES):
        to_core(k).wait_send()
        to_far(k).wait_send()
        to_near(k).wait_send()
        share(0, side, k).wait_send()
        share(1, side, k).wait_send()
    base_copy.wait_send()

    @pl.loop(1, outer)
    def _(d):
        query_copy(d).wait_send()
        stat_copy(d).wait()

    every = [stat_recv[d] for d in range(outer)]
    overall = functools.reduce(jnp.maximum, [s[:1, :] for s in every])
    shares = [jnp.exp(s[:1, :] - overall) * s[4:5, :] for s in every]
    inverse = 1.0 / functools.reduce(jnp.add, shares)

    def column(d):
        across = jnp.broadcast_to(shares[d] * inverse, (LANES, shares[d].shape[1]))
        return jnp.transpose(across)[:rows, :1]

    acc[0] = acc[0] * column(0)
    for d in range(1, outer):
        part_copy(d).wait()
        acc[0] += part_recv[d].astype(jnp.float32) * column(d)
    for h in range(local):
        out_ref[:, h * LAT : (h + 1) * LAT] = acc[0, h * count : (h + 1) * count, :].astype(
            out_ref.dtype
        )


def on_device(latents, queries, hot_ids, lengths):
    width = LAT + ROPE
    n_rep = lax.axis_size("rep")
    n_ctx = lax.axis_size("ctx")
    count = queries.shape[0]
    local = queries.shape[1] // width
    rows = count * local
    outer = n_ctx // 2
    wide = -(-rows // LANES) * LANES
    piece = BLK // PIECES
    sems = 5 * PIECES + 3 * outer
    vmem = pl.BlockSpec(memory_space=pltpu.VMEM)
    smem = pl.BlockSpec(memory_space=pltpu.SMEM)
    bf16, f32 = jnp.bfloat16, jnp.float32
    return pl.pallas_call(
        functools.partial(kernel, n_ctx, n_rep),
        out_shape=jax.ShapeDtypeStruct((count, local * LAT), bf16),
        in_specs=[vmem, vmem, smem, smem],
        out_specs=vmem,
        scratch_shapes=[
            pltpu.VMEM((PIECES, width, piece), bf16),
            pltpu.VMEM((PIECES, width, piece), bf16),
            pltpu.VMEM((PIECES, width, piece), bf16),
            pltpu.VMEM((PIECES, width, piece), bf16),
            pltpu.VMEM((2, HOT_GRP, PIECES, width, piece), bf16),
            pltpu.VMEM((outer, rows, width), bf16),
            pltpu.VMEM((8, LANES), jnp.int32),
            pltpu.VMEM((8, LANES), jnp.int32),
            pltpu.VMEM((outer, 8, wide), f32),
            pltpu.VMEM((outer, 8, wide), f32),
            pltpu.VMEM((outer, rows, LAT), bf16),
            pltpu.VMEM((outer, rows, LAT), bf16),
            pltpu.VMEM((outer, rows, LAT), f32),
            pltpu.VMEM((outer, rows, LANES), f32),
            pltpu.VMEM((outer, rows, LANES), f32),
            pltpu.SemaphoreType.DMA((sems,)),
            pltpu.SemaphoreType.DMA((sems,)),
        ],
        compiler_params=pltpu.CompilerParams(
            collective_id=0, has_side_effects=True, vmem_limit_bytes=56 * 1024 * 1024
        ),
    )(latents.T, queries, hot_ids, lengths)


def solution(mesh):
    placed = (P(("ctx", "rep"), None), P("rep", "ctx"), P("ctx"), P("rep"))
    return jax.shard_map(
        on_device, mesh=mesh, in_specs=placed, out_specs=P("rep", "ctx"), check_vma=False
    )
```

```python
import functools

import jax
import jax.numpy as jnp
from jax import lax
from jax.experimental import pallas as pl
from jax.experimental.pallas import tpu as pltpu
from jax.sharding import PartitionSpec as P

H = 128
LAT = 512
ROPE = 64
QK = 192
BLK = 1024
HOT_GRP = 2
LANES = 128
PIECES = 8
SPAN = 1024
MESH = pl.DeviceIdType.MESH


def kernel(
    n_ctx, n_rep, latent_ref, query_ref, hot_ref, length_ref, out_ref,
    cand, from_core, merged, from_far, keys, heads, base_own, base_near, stat_send, stat_recv,
    part_send, part_recv, acc, peaks, totals, send_sem, recv_sem,
):
    outer = n_ctx // 2
    count = query_ref.shape[0]
    width = latent_ref.shape[0]
    local = query_ref.shape[1] // width
    rows = count * local
    per_device = latent_ref.shape[1] // BLK
    piece = BLK // PIECES
    group = lax.axis_index("ctx")
    rep = lax.axis_index("rep")
    side = lax.rem(rep, 2)
    core = {"rep": rep + 1 - 2 * side}
    far = {"rep": lax.rem(rep + n_rep // 2, n_rep)}
    near = {"ctx": group + 1 - 2 * lax.rem(group, 2)}

    def line(d):
        return {"ctx": lax.rem(group + 2 * d, n_ctx)}

    barrier = pltpu.get_barrier_semaphore()
    for target in (core, far, near):
        pl.semaphore_signal(barrier, inc=1, device_id=target, device_id_type=MESH)

    @pl.loop(1, outer)
    def _(d):
        pl.semaphore_signal(barrier, inc=1, device_id=line(d), device_id_type=MESH)

    def factors(slot):
        hot = jnp.full((1, LANES), hot_ref[slot], jnp.int32)
        return [
            jnp.where(hot == rep * per_device + b, 1.0, 0.0).astype(jnp.bfloat16)
            for b in range(per_device)
        ]

    other_factors = factors(1 - side)
    own_factors = factors(side)

    def held(chosen, k):
        return functools.reduce(
            jnp.add,
            [
                latent_ref[:, b * BLK + k * piece : b * BLK + (k + 1) * piece] * chosen[b]
                for b in range(per_device)
            ],
        )

    cand[0] = held(other_factors, 0)
    pl.semaphore_wait(barrier, outer + 2)

    def copy(src, dst, sem, target):
        return pltpu.make_async_remote_copy(
            src_ref=src, dst_ref=dst, send_sem=send_sem.at[sem], recv_sem=recv_sem.at[sem],
            device_id=target, device_id_type=MESH,
        )

    def to_core(k):
        return copy(cand.at[k], from_core.at[k], k, core)

    def to_far(k):
        return copy(merged.at[k], from_far.at[k], PIECES + k, far)

    def to_near(k):
        return copy(keys.at[0, side, k], keys.at[1, side, k], 2 * PIECES + k, near)

    def share(where, slot, k):
        ref = keys.at[where, slot, k]
        return copy(ref, ref, (3 + where) * PIECES + k, core)

    first = 5 * PIECES
    base_copy = copy(base_own, base_near, first, near)

    def query_copy(d):
        return copy(heads.at[0], heads.at[d], first + d, line(d))

    def part_copy(d):
        return copy(part_send.at[d], part_recv.at[d], first + outer + d, line(outer - d))

    def stat_copy(d):
        return copy(stat_send.at[d], stat_recv.at[d], first + 2 * outer + d, line(outer - d))

    to_core(0).start()
    for k in range(1, PIECES):
        cand[k] = held(other_factors, k)
        to_core(k).start()
    for h in range(local):
        heads[0, h * count : (h + 1) * count, :] = query_ref[:, h * width : (h + 1) * width]
    slot_row = lax.broadcasted_iota(jnp.int32, (8, LANES), 0)
    base = jnp.zeros((8, LANES), jnp.int32)
    for slot in range(HOT_GRP):
        at = (group * (n_rep * per_device) + hot_ref[slot]) * BLK
        base = jnp.where(slot_row == slot, at, base)
    base_own[...] = base

    for k in range(PIECES):
        to_core(k).wait_recv()
        merged[k] = held(own_factors, k) + from_core[k]
        to_far(k).start()
        if k == 0:
            @pl.loop(1, outer)
            def _(d):
                query_copy(d).start()
            base_copy.start()

    query_row = lax.broadcasted_iota(jnp.int32, (count, LANES), 0)
    limit = jnp.zeros((count, LANES), jnp.int32)
    for q in range(count):
        limit = jnp.where(query_row == q, length_ref[q], limit)
    limits = jnp.concatenate([limit] * local, axis=0)[:, :1]

    acc[...] = jnp.zeros_like(acc)
    peaks[...] = jnp.full_like(peaks, -1e30)
    totals[...] = jnp.zeros_like(totals)
    per_span = SPAN // piece

    def absorb(d, where, slot, span):
        key_cols = jnp.concatenate(
            [keys[where, slot, span * per_span + i] for i in range(per_span)], axis=1
        )
        score = jnp.dot(
            heads[d], key_cols, preferred_element_type=jnp.float32
        ) * (QK ** (-0.5))
        ref = base_own if where == 0 else base_near
        base = jnp.concatenate([ref[slot : slot + 1, :]] * (SPAN // LANES), axis=1)
        position = base + span * SPAN + lax.broadcasted_iota(jnp.int32, (1, SPAN), 1)
        visible = position < limits
        score = jnp.where(visible, score, -1e30)
        old = peaks[d]
        new = jnp.maximum(old, jnp.max(score, axis=1, keepdims=True))
        weight = jnp.exp(jnp.where(visible, score - new[:, :1], -1e30)).astype(jnp.bfloat16)
        shrink = jnp.exp(old - new)
        peaks[d] = new
        totals[d] = totals[d] * shrink + jnp.sum(
            weight.astype(jnp.float32), axis=1, keepdims=True
        )
        acc[d] = acc[d] * shrink[:, :1] + lax.dot_general(
            weight, key_cols[:LAT, :], (((1,), (1,)), ((), ())),
            preferred_element_type=jnp.float32,
        )

    def absorb_rest(where, slot, span):
        @pl.loop(1, outer)
        def _(d):
            absorb(d, where, slot, span)

    def finish(d):
        total = totals[d]
        lane = lax.broadcasted_iota(jnp.int32, (rows, LANES), 1)
        stats = jnp.where(lane < 4, peaks[d], total)
        if rows % LANES:
            stats = jnp.concatenate(
                [stats, jnp.zeros((LANES - rows % LANES, LANES), jnp.float32)], axis=0
            )
        inverse = 1.0 / jnp.maximum(total, 1e-30)
        return acc[d] * inverse[:, :1], jnp.transpose(stats)[:8, :]

    def pass_on(k):
        to_near(k).wait_recv()
        share(1, side, k).start()

    base_copy.wait_recv()
    for k in range(PIECES):
        to_far(k).wait_recv()
        keys[0, side, k] = merged[k] + from_far[k]
        to_near(k).start()
        share(0, side, k).start()
        if k >= 2:
            pass_on(k - 2)
    for k in range(PIECES):
        share(0, 1 - side, k).wait_recv()
    spans = BLK // SPAN
    for slot in range(HOT_GRP):
        for span in range(spans):
            absorb(0, 0, slot, span)

    @pl.loop(1, outer)
    def _(d):
        query_copy(d).wait_recv()

    for slot in range(HOT_GRP):
        pass_on(PIECES - HOT_GRP + slot)
        for span in range(spans):
            absorb_rest(0, slot, span)
    for k in range(PIECES):
        share(1, 1 - side, k).wait_recv()

    @pl.loop(1, outer)
    def _(d):
        for slot in range(HOT_GRP):
            for span in range(spans):
                absorb(d, 1, slot, span)
        part, stats = finish(d)
        stat_send[d] = stats
        part_send[d] = part.astype(jnp.bfloat16)
        stat_copy(d).start()
        part_copy(d).start()

    for slot in range(HOT_GRP):
        for span in range(spans):
            absorb(0, 1, slot, span)
    part, stats = finish(0)
    acc[0] = part
    stat_recv[0] = stats

    for k in range(PIECES):
        to_core(k).wait_send()
        to_far(k).wait_send()
        to_near(k).wait_send()
        share(0, side, k).wait_send()
        share(1, side, k).wait_send()
    base_copy.wait_send()

    @pl.loop(1, outer)
    def _(d):
        query_copy(d).wait_send()
        stat_copy(d).wait()

    every = [stat_recv[d] for d in range(outer)]
    overall = functools.reduce(jnp.maximum, [s[:1, :] for s in every])
    shares = [jnp.exp(s[:1, :] - overall) * s[4:5, :] for s in every]
    inverse = 1.0 / functools.reduce(jnp.add, shares)

    def column(d):
        across = jnp.broadcast_to(shares[d] * inverse, (LANES, shares[d].shape[1]))
        return jnp.transpose(across)[:rows, :1]

    acc[0] = acc[0] * column(0)
    for d in range(1, outer):
        part_copy(d).wait()
        acc[0] += part_recv[d].astype(jnp.float32) * column(d)
    for h in range(local):
        out_ref[:, h * LAT : (h + 1) * LAT] = acc[0, h * count : (h + 1) * count, :].astype(
            out_ref.dtype
        )


def on_device(latents, queries, hot_ids, lengths):
    width = LAT + ROPE
    n_rep = lax.axis_size("rep")
    n_ctx = lax.axis_size("ctx")
    count = queries.shape[0]
    local = queries.shape[1] // width
    rows = count * local
    outer = n_ctx // 2
    wide = -(-rows // LANES) * LANES
    piece = BLK // PIECES
    sems = 5 * PIECES + 3 * outer
    vmem = pl.BlockSpec(memory_space=pltpu.VMEM)
    smem = pl.BlockSpec(memory_space=pltpu.SMEM)
    bf16, f32 = jnp.bfloat16, jnp.float32
    return pl.pallas_call(
        functools.partial(kernel, n_ctx, n_rep),
        out_shape=jax.ShapeDtypeStruct((count, local * LAT), bf16),
        in_specs=[vmem, vmem, smem, smem],
        out_specs=vmem,
        scratch_shapes=[
            pltpu.VMEM((PIECES, width, piece), bf16),
            pltpu.VMEM((PIECES, width, piece), bf16),
            pltpu.VMEM((PIECES, width, piece), bf16),
            pltpu.VMEM((PIECES, width, piece), bf16),
            pltpu.VMEM((2, HOT_GRP, PIECES, width, piece), bf16),
            pltpu.VMEM((outer, rows, width), bf16),
            pltpu.VMEM((8, LANES), jnp.int32),
            pltpu.VMEM((8, LANES), jnp.int32),
            pltpu.VMEM((outer, 8, wide), f32),
            pltpu.VMEM((outer, 8, wide), f32),
            pltpu.VMEM((outer, rows, LAT), bf16),
            pltpu.VMEM((outer, rows, LAT), bf16),
            pltpu.VMEM((outer, rows, LAT), f32),
            pltpu.VMEM((outer, rows, LANES), f32),
            pltpu.VMEM((outer, rows, LANES), f32),
            pltpu.SemaphoreType.DMA((sems,)),
            pltpu.SemaphoreType.DMA((sems,)),
        ],
        compiler_params=pltpu.CompilerParams(
            collective_id=0, has_side_effects=True, vmem_limit_bytes=56 * 1024 * 1024
        ),
    )(latents.T, queries, hot_ids, lengths)


def solution(mesh):
    placed = (P(("ctx", "rep"), None), P("rep", "ctx"), P("ctx"), P("rep"))
    return jax.shard_map(
        on_device, mesh=mesh, in_specs=placed, out_specs=P("rep", "ctx"), check_vma=False
    )
```
